16 devices in a mesh: tp: 2 (over z), dp: 8 (over y, x, core).
Axes of the slice: x: 2, y: 2, z: 2, core: 2. Of those that a mesh axis runs over, the one named last changes fastest.
Arguments:
- hidden: bfloat16 [24, 384, 512], P('dp')
- labels: int32 [24, 384], P('dp')
- loss_mask: int32 [24, 384], P('dp')
- ln_gain: float32 [512], replicated
- ln_bias: float32 [512], replicated
- w_query: bfloat16 [512, 8, 64], P(None, 'tp')
- w_key: bfloat16 [512, 8, 64], P(None, 'tp')
- w_value: bfloat16 [512, 8, 64], P(None, 'tp')
- w_attn_out: bfloat16 [8, 64, 512], P('tp')
- w_fc_in: bfloat16 [512, 2048], P(None, 'tp')
- b_fc_in: float32 [2048], P('tp')
- w_fc_out: bfloat16 [2048, 512], P('tp')
- b_fc_out: float32 [512], replicated
- lnf_gain: float32 [512], replicated
- lnf_bias: float32 [512], replicated
- w_head: bfloat16 [512, 50304], P(None, 'tp')
- b_head: float32 [50304], P('tp')
Outputs:
- output 1: float32 [], replicated
- output 2: bfloat16 [24, 384, 512], P('dp')
- output 3: float32 [512], replicated
- output 4: float32 [512], replicated
- output 5: float32 [512, 8, 64], P(None, 'tp')
- output 6: float32 [512, 8, 64], P(None, 'tp')
- output 7: float32 [512, 8, 64], P(None, 'tp')
- output 8: float32 [8, 64, 512], P('tp')
- output 9: float32 [512, 2048], P(None, 'tp')
- output 10: float32 [2048], P('tp')
- output 11: float32 [2048, 512], P('tp')
- output 12: float32 [512], replicated
- output 13: float32 [512], replicated
- output 14: float32 [512], replicated
- output 15: float32 [512, 50304], P(None, 'tp')
- output 16: float32 [50304], P('tp')
All inputs are finite; a program needn't handle non-finite values.
Results may differ from the reference program's by a relative error of at most 0.0140425.
Values sent between devices are 32-bit elements.
A program may use at most 1 GiB of HBM per device.

```python
import jax
import jax.numpy as jnp
from jax import lax

BATCH_ROWS = 24
SEQ_LEN = 384
D_MODEL = 512
N_HEADS = 8
HEAD_DIM = 64
FF_DIM = 2048
VOCAB_SIZE = 50304
ROT_DIM = HEAD_DIM // 4
LN_EPS = 1e-5
ROPE_BASE = 10000.0


def setup_inputs(seed: int = 0) -> dict:
    keys = jax.random.split(jax.random.key(seed), 17)

    def normal(index, shape, scale):
        return jax.random.normal(keys[index], shape, jnp.float32) * scale

    row_ids = jnp.arange(BATCH_ROWS)
    lengths = jax.random.randint(keys[1], (BATCH_ROWS,), SEQ_LEN // 8, SEQ_LEN + 1)
    lengths = jnp.where(row_ids == 0, SEQ_LEN, lengths)
    lengths = jnp.where(row_ids == BATCH_ROWS - 1, SEQ_LEN // 8, lengths)
    loss_mask = (jnp.arange(SEQ_LEN)[None, :] < lengths[:, None]).astype(jnp.int32)
    labels = jax.random.randint(keys[2], (BATCH_ROWS, SEQ_LEN), 0, VOCAB_SIZE)
    labels = labels.at[0, 0].set(0).at[0, 1].set(VOCAB_SIZE - 1)
    d_scale = D_MODEL ** -0.5
    return {
        'hidden': normal(0, (BATCH_ROWS, SEQ_LEN, D_MODEL), 1.0).astype(jnp.bfloat16),
        'labels': labels,
        'loss_mask': loss_mask,
        'ln_gain': 1.0 + normal(3, (D_MODEL,), 0.3),
        'ln_bias': normal(4, (D_MODEL,), 0.3),
        'w_query': normal(5, (D_MODEL, N_HEADS, HEAD_DIM), d_scale).astype(jnp.bfloat16),
        'w_key': normal(6, (D_MODEL, N_HEADS, HEAD_DIM), d_scale).astype(jnp.bfloat16),
        'w_value': normal(7, (D_MODEL, N_HEADS, HEAD_DIM), d_scale).astype(jnp.bfloat16),
        'w_attn_out': normal(8, (N_HEADS, HEAD_DIM, D_MODEL), d_scale).astype(jnp.bfloat16),
        'w_fc_in': normal(9, (D_MODEL, FF_DIM), d_scale).astype(jnp.bfloat16),
        'b_fc_in': normal(10, (FF_DIM,), 0.5),
        'w_fc_out': normal(11, (FF_DIM, D_MODEL), FF_DIM ** -0.5).astype(jnp.bfloat16),
        'b_fc_out': normal(12, (D_MODEL,), 0.5),
        'lnf_gain': 1.0 + normal(13, (D_MODEL,), 0.3),
        'lnf_bias': normal(14, (D_MODEL,), 0.3),
        'w_head': normal(15, (D_MODEL, VOCAB_SIZE), d_scale).astype(jnp.bfloat16),
        'b_head': normal(16, (VOCAB_SIZE,), 1.0) + jnp.linspace(-3.0, 3.0, VOCAB_SIZE),
    }


def bf16_grid(values):
    return values.astype(jnp.bfloat16).astype(jnp.float32)


def layer_norm(values, gain_vec, shift_vec):
    row_mean = jnp.mean(values, axis=-1, keepdims=True)
    centered = values - row_mean
    variance = jnp.mean(centered * centered, axis=-1, keepdims=True)
    return centered * lax.rsqrt(variance + LN_EPS) * gain_vec + shift_vec


def rope_tables(seq_count, rot_dim):
    half_rot = rot_dim // 2
    inv_freq = ROPE_BASE ** (-2.0 * jnp.arange(half_rot, dtype=jnp.float32) / rot_dim)
    angles = jnp.arange(seq_count, dtype=jnp.float32)[:, None] * inv_freq[None, :]
    return jnp.cos(angles)[:, None, :], jnp.sin(angles)[:, None, :]


def apply_rotary(tensor, cosine, sine_tab):
    rot_dim = 2 * cosine.shape[-1]
    pairs = tensor[..., :rot_dim].reshape(tensor.shape[:-1] + (rot_dim // 2, 2))
    even_part = pairs[..., 0]
    odd_part = pairs[..., 1]
    rotated = jnp.stack([even_part * cosine - odd_part * sine_tab, odd_part * cosine + even_part * sine_tab], axis=-1)
    return jnp.concatenate([rotated.reshape(tensor.shape[:-1] + (rot_dim,)), tensor[..., rot_dim:]], axis=-1)


def row_loss(params, hidden_row, label_row, mask_row, inv_count):
    (ln_gain, ln_bias, w_query, w_key, w_value, w_attn_out, w_fc_in, b_fc_in,
     w_fc_out, b_fc_out, lnf_gain, lnf_bias, w_head, b_head) = params
    seq_count = hidden_row.shape[0]
    cosine, sine_tab = rope_tables(seq_count, ROT_DIM)
    normed = bf16_grid(layer_norm(hidden_row, ln_gain, ln_bias))
    q_rot = bf16_grid(apply_rotary(jnp.einsum('td,dhe->the', normed, w_query), cosine, sine_tab))
    k_rot = bf16_grid(apply_rotary(jnp.einsum('td,dhe->the', normed, w_key), cosine, sine_tab))
    v_proj = bf16_grid(jnp.einsum('td,dhe->the', normed, w_value))
    causal = jnp.arange(seq_count)[None, :] <= jnp.arange(seq_count)[:, None]
    scores = jnp.einsum('qhe,khe->hqk', q_rot, k_rot) * (HEAD_DIM ** -0.5)
    probs = bf16_grid(jax.nn.softmax(jnp.where(causal[None], scores, -1e30), axis=-1))
    context = bf16_grid(jnp.einsum('hqk,khe->qhe', probs, v_proj))
    attn_out = jnp.einsum('qhe,hed->qd', context, w_attn_out)
    gelu_out = bf16_grid(jax.nn.gelu(jnp.dot(normed, w_fc_in) + b_fc_in, approximate=True))
    resid_out = hidden_row + attn_out + jnp.dot(gelu_out, w_fc_out) + b_fc_out
    final_norm = bf16_grid(layer_norm(resid_out, lnf_gain, lnf_bias))
    logits = jnp.dot(final_norm, w_head) + b_head
    log_norm = jax.nn.logsumexp(logits, axis=-1)
    target_logit = jnp.take_along_axis(logits, label_row[:, None], axis=-1)[:, 0]
    return jnp.sum(mask_row.astype(jnp.float32) * (log_norm - target_logit)) * inv_count


def reference(hidden, labels, loss_mask, ln_gain, ln_bias, w_query, w_key, w_value, w_attn_out,
              w_fc_in, b_fc_in, w_fc_out, b_fc_out, lnf_gain, lnf_bias, w_head, b_head):
    params = tuple(leaf.astype(jnp.float32) for leaf in (
        ln_gain, ln_bias, w_query, w_key, w_value, w_attn_out, w_fc_in, b_fc_in,
        w_fc_out, b_fc_out, lnf_gain, lnf_bias, w_head, b_head))
    inv_count = 1.0 / jnp.sum(loss_mask.astype(jnp.float32))
    checked = jax.checkpoint(row_loss)

    def total_loss(param_tuple, hidden_f32):
        per_row = lax.map(
            lambda row_args: checked(param_tuple, row_args[0], row_args[1], row_args[2], inv_count),
            (hidden_f32, labels, loss_mask))
        return jnp.sum(per_row)

    loss, vjp_fn = jax.vjp(total_loss, params, hidden.astype(jnp.float32))
    grads, grad_hidden = vjp_fn(jnp.ones_like(loss))
    (g_ln_gain, g_ln_bias, g_w_query, g_w_key, g_w_value, g_w_attn_out, g_w_fc_in, g_b_fc_in,
     g_w_fc_out, g_b_fc_out, g_lnf_gain, g_lnf_bias, g_w_head, g_b_head) = grads
    return (loss, grad_hidden.astype(jnp.bfloat16), g_ln_gain, g_ln_bias, g_w_query, g_w_key, g_w_value,
            g_w_attn_out, g_w_fc_in, g_b_fc_in, g_w_fc_out, g_b_fc_out, g_lnf_gain, g_lnf_bias,
            g_w_head, g_b_head)
```

```python
import functools
import jax
import jax.numpy as jnp
from jax import lax
from jax.experimental import pallas as pl
from jax.experimental.pallas import tpu as pltpu
from jax.sharding import PartitionSpec as P

SEQ = 384
D = 512
FC = 2560
FR = 320
GC = 1056
GB = 1152
GS = 48
GR = 768
PAD_BIAS = -3e38
PAD_LSE = 1e30
PAD_LABEL = -1e9
VMEM_LIMIT = 63 * 1024 * 1024


def head_kernel(n_col, tail, seqs, off_ref, z_ref, w_ref, wt_ref, b_ref, u_ref, m_out, s_out, zc, acc, m_run, s_run, lbuf):
    col = pl.program_id(0)
    n_rows = (off_ref[seqs] + FR - 1) // FR

    @pl.when(col == 0)
    def _():
        zc[...] = jnp.zeros_like(zc)
        for i in range(seqs):
            zc[pl.ds(pl.multiple_of(off_ref[i], 16), SEQ), :] = z_ref[i]
        acc[...] = jnp.zeros_like(acc)
        s_run[...] = jnp.zeros_like(s_run)
        m_run[...] = jnp.full_like(m_run, PAD_BIAS)

    @pl.when(col == n_col - 1)
    def _():
        w_ref[:, tail:] = jnp.zeros((D, FC - tail), jnp.bfloat16)
        wt_ref[tail:, :] = jnp.zeros((FC - tail, D), jnp.bfloat16)

    def logits(step, slot):
        rows = pl.ds(pl.multiple_of(step * FR, FR), FR)
        lbuf[slot] = jnp.dot(zc[rows, :], w_ref[...], preferred_element_type=jnp.float32) + b_ref[...]

    def process(step, slot):
        rows = pl.ds(pl.multiple_of(step * FR, FR), FR)
        vals = lbuf[slot]
        m_old = m_run[rows, :]
        m_new = jnp.maximum(m_old, jnp.max(vals, axis=-1, keepdims=True))
        alpha = jnp.exp(m_old - m_new)
        parts = [jnp.exp(vals[:, c * 128:(c + 1) * 128] - m_new) for c in range(FC // 128)]
        s_run[rows, :] = s_run[rows, :] * alpha + functools.reduce(jnp.add, parts)
        m_run[rows, :] = m_new
        p = jnp.concatenate([part.astype(jnp.bfloat16) for part in parts], axis=-1)
        new = jnp.dot(p, wt_ref[...], preferred_element_type=jnp.float32)
        acc[rows, :] = acc[rows, :] * jnp.concatenate([alpha] * (D // 128), axis=-1) + new

    logits(0, 0)

    def body(step, carry):
        slot = lax.rem(step, 2)
        logits(step + 1, 1 - slot)
        process(step, slot)
        return carry

    lax.fori_loop(0, n_rows - 1, body, 0)
    process(n_rows - 1, lax.rem(n_rows - 1, 2))

    @pl.when(col == n_col - 1)
    def _():
        for i in range(seqs):
            rows = pl.ds(pl.multiple_of(off_ref[i], 16), SEQ)
            u_ref[i] = acc[rows, :]
            m_out[i] = m_run[rows, :]
            s_out[i] = jnp.broadcast_to(jnp.sum(s_run[rows, :], axis=-1, keepdims=True), (SEQ, 128))


def head_forward(off, z, w, wt, b):
    seqs = z.shape[0]
    vocab = wt.shape[0]
    n_col = pl.cdiv(vocab, FC)
    rows = seqs * SEQ + 384
    rows = (rows + FR - 1) // FR * FR
    whole = lambda shape: pl.BlockSpec(shape, lambda j, off: (0,) * len(shape))
    return pl.pallas_call(
        functools.partial(head_kernel, n_col, vocab - (n_col - 1) * FC, seqs),
        grid_spec=pltpu.PrefetchScalarGridSpec(
            num_scalar_prefetch=1,
            grid=(n_col,),
            in_specs=[whole((seqs, SEQ, D)), pl.BlockSpec((D, FC), lambda j, off: (0, j)),
                      pl.BlockSpec((FC, D), lambda j, off: (j, 0)), pl.BlockSpec((1, FC), lambda j, off: (0, j))],
            out_specs=[whole((seqs, SEQ, D)), whole((seqs, SEQ, 128)), whole((seqs, SEQ, 128))],
            scratch_shapes=[pltpu.VMEM((rows, D), jnp.bfloat16), pltpu.VMEM((rows, D), jnp.float32),
                            pltpu.VMEM((rows, 128), jnp.float32), pltpu.VMEM((rows, 128), jnp.float32),
                            pltpu.VMEM((2, FR, FC), jnp.float32)]),
        out_shape=[jax.ShapeDtypeStruct((seqs, SEQ, D), jnp.float32), jax.ShapeDtypeStruct((seqs, SEQ, 128), jnp.float32),
                   jax.ShapeDtypeStruct((seqs, SEQ, 128), jnp.float32)],
        compiler_params=pltpu.CompilerParams(dimension_semantics=("arbitrary",), vmem_limit_bytes=VMEM_LIMIT),
        cost_estimate=pl.CostEstimate(flops=4 * 900 * D * vocab, bytes_accessed=4 * D * vocab, transcendentals=900 * vocab),
        name="head_forward",
    )(off, z, w, wt, b)


def prep_kernel(seqs, off_ref, *refs):
    (*pieces, lse_in, lab_in, zc_out, zt_out, lse_out, lab_out,
     stage, zc, zt, lse_v, lab_v, lse, lab, lse_t, lab_t, sems) = refs
    n_seq = seqs * 8
    half = SEQ // 2
    n_blk = (off_ref[n_seq] + GR - 1) // GR

    def fetch(seq):
        piece, row = divmod(seq, seqs)
        slot = seq % 2
        if piece < 6:
            return [pltpu.make_async_copy(pieces[piece].at[row], stage.at[slot], sems.at[slot])]
        return [pltpu.make_async_copy(pieces[2 * piece - 6 + k].at[row], stage.at[slot, pl.ds(k * half, half)],
                                      sems.at[slot + 2 * k]) for k in range(2)]

    stats = [pltpu.make_async_copy(lse_in, lse_v, sems.at[4]), pltpu.make_async_copy(lab_in, lab_v, sems.at[5])]
    for copy in fetch(0) + fetch(1) + stats:
        copy.start()
    zc[...] = jnp.zeros_like(zc)
    lse[...] = jnp.full_like(lse, PAD_LSE)
    lab[...] = jnp.full_like(lab, PAD_LABEL)
    for seq in range(n_seq):
        for copy in fetch(seq):
            copy.wait()
        zc[pl.ds(pl.multiple_of(off_ref[seq], 16), SEQ), :] = stage[seq % 2].astype(jnp.bfloat16)
        if seq + 2 < n_seq:
            for copy in fetch(seq + 2):
                copy.start()

    def out_z(step):
        rows = pl.ds(pl.multiple_of(step * GR, GR), GR)
        return [pltpu.make_async_copy(zc.at[rows, :], zc_out.at[rows, :], sems.at[0]),
                pltpu.make_async_copy(zt.at[:, rows], zt_out.at[:, rows], sems.at[1])]

    def out_stats(step):
        rows = pl.ds(pl.multiple_of(step * GR, GR), GR)
        return [pltpu.make_async_copy(lse_t.at[:, rows], lse_out.at[:, rows], sems.at[2]),
                pltpu.make_async_copy(lab_t.at[:, rows], lab_out.at[:, rows], sems.at[3])]

    def turn(step, carry):
        rows = pl.ds(pl.multiple_of(step * GR, GR), GR)
        zt[:, rows] = zc[rows, :].T
        for copy in out_z(step):
            copy.start()
        return carry

    lax.fori_loop(0, n_blk, turn, 0)
    for copy in stats:
        copy.wait()
    for seq in range(n_seq):
        rows = pl.ds(pl.multiple_of(off_ref[seq], 16), SEQ)
        lse[rows, :] = lse_v[seq]
        lab[rows, :] = lab_v[seq]

    def send(step, carry):
        rows = pl.ds(pl.multiple_of(step * GR, GR), GR)
        lse_t[:, rows] = lse[rows, :].T[:8]
        lab_t[:, rows] = lab[rows, :].T[:8]
        for copy in out_stats(step):
            copy.start()
        return carry

    def finish(step, carry):
        for copy in out_z(step) + out_stats(step):
            copy.wait()
        return carry

    lax.fori_loop(0, n_blk, send, 0)
    lax.fori_loop(0, n_blk, finish, 0)


def prep(off, pieces, lse, lab):
    n_seq = lse.shape[0]
    rows = n_seq * SEQ
    any_spec = pl.BlockSpec(memory_space=pl.ANY)
    return pl.pallas_call(
        functools.partial(prep_kernel, n_seq // 8),
        grid_spec=pltpu.PrefetchScalarGridSpec(
            num_scalar_prefetch=1, grid=(1,), in_specs=[any_spec] * (len(pieces) + 2), out_specs=[any_spec] * 4,
            scratch_shapes=[pltpu.VMEM((2, SEQ, D), jnp.float32), pltpu.VMEM((rows, D), jnp.bfloat16),
                            pltpu.VMEM((D, rows), jnp.bfloat16), pltpu.VMEM((n_seq, SEQ, 128), jnp.float32),
                            pltpu.VMEM((n_seq, SEQ, 128), jnp.float32), pltpu.VMEM((rows, 128), jnp.float32),
                            pltpu.VMEM((rows, 128), jnp.float32), pltpu.VMEM((8, rows), jnp.float32),
                            pltpu.VMEM((8, rows), jnp.float32), pltpu.SemaphoreType.DMA((6,))]),
        out_shape=[jax.ShapeDtypeStruct((rows, D), jnp.bfloat16), jax.ShapeDtypeStruct((D, rows), jnp.bfloat16),
                   jax.ShapeDtypeStruct((8, rows), jnp.float32), jax.ShapeDtypeStruct((8, rows), jnp.float32)],
        compiler_params=pltpu.CompilerParams(dimension_semantics=("arbitrary",), vmem_limit_bytes=VMEM_LIMIT),
        cost_estimate=pl.CostEstimate(flops=400 * rows * 128, bytes_accessed=8 * rows * D, transcendentals=0),
        name="prep",
    )(off, *pieces, lse, lab)


def grad_head_kernel(sc_ref, wgt_ref, z_hbm, zt_hbm, lse_hbm, lab_hbm, wt_ref, b_ref, *refs):
    (out_ref, send_ref, gb_ref, zc, zt, lse, lab, lbuf, pbuf, bias, sems) = refs[-11:]
    j = pl.program_id(0)
    n_blk = (sc_ref[0] + GR - 1) // GR
    row0 = ((sc_ref[1] + j) * GC).astype(jnp.float32)
    weight = wgt_ref[0]

    @pl.when(j == 0)
    def _():
        def copies(step):
            cols = pl.ds(pl.multiple_of(step * GR, GR), GR)
            return [pltpu.make_async_copy(z_hbm.at[cols, :], zc.at[cols, :], sems.at[0]),
                    pltpu.make_async_copy(zt_hbm.at[:, cols], zt.at[:, cols], sems.at[1]),
                    pltpu.make_async_copy(lse_hbm.at[:, cols], lse.at[:, cols], sems.at[2]),
                    pltpu.make_async_copy(lab_hbm.at[:, cols], lab.at[:, cols], sems.at[3])]

        def start(step, carry):
            for copy in copies(step):
                copy.start()
            return carry

        def wait(step, carry):
            for copy in copies(step):
                copy.wait()
            return carry
        lax.fori_loop(0, n_blk, start, 0)
        lax.fori_loop(0, n_blk, wait, 0)

    iota = lax.broadcasted_iota(jnp.int32, (GS, 128), 0).astype(jnp.float32)
    for c in range(GB // 128):
        cols = slice(c * 128, (c + 1) * 128)
        bias[cols, :] = jnp.broadcast_to(b_ref[0, :, cols], (128, 128)).T

    def logits(step, slot):
        cols = pl.ds(pl.multiple_of(step * GR, GR), GR)
        lbuf[slot] = jnp.dot(wt_ref[...], zt[:, cols], preferred_element_type=jnp.float32)

    def process(step, slot):
        for s in range(GC // GS):
            strip = slice(s * GS, (s + 1) * GS)
            shift = bias[strip, :]
            total = None
            for c in range(GR // 128):
                cols = pl.ds(pl.multiple_of(step * GR + c * 128, 128), 128)
                p = jnp.exp(lbuf[slot, strip, c * 128:(c + 1) * 128] + shift - lse[0:1, cols])
                p = jnp.where(iota == lab[0:1, cols] - (row0 + s * GS), p - weight, p)
                total = p if total is None else total + p
                pbuf[strip, c * 128:(c + 1) * 128] = p.astype(jnp.bfloat16)
            gb_ref[strip, :] += total
        rows = pl.ds(pl.multiple_of(step * GR, GR), GR)
        out_ref[...] += jnp.dot(pbuf[...], zc[rows, :], preferred_element_type=jnp.float32)

    out_ref[...] = jnp.zeros_like(out_ref)
    gb_ref[...] = jnp.zeros_like(gb_ref)
    logits(0, 0)

    def body(step, carry):
        slot = lax.rem(step, 2)
        logits(step + 1, 1 - slot)
        process(step, slot)
        return carry

    lax.fori_loop(0, n_blk - 1, body, 0)
    process(n_blk - 1, lax.rem(n_blk - 1, 2))
    send_ref[...] = out_ref[...]


def grad_head(count, sc, wgt, zc, zt, lse, lab, wt, b_blk, full=None):
    rows = zc.shape[0]
    any_spec = pl.BlockSpec(memory_space=pl.ANY)
    smem = pl.BlockSpec(memory_space=pltpu.SMEM)
    extra = [] if full is None else [full]
    mine = lambda j, sc: (sc[1] + j, 0)
    return pl.pallas_call(
        grad_head_kernel,
        grid_spec=pltpu.PrefetchScalarGridSpec(
            num_scalar_prefetch=1, grid=(count,),
            in_specs=[smem, any_spec, any_spec, any_spec, any_spec, pl.BlockSpec((GC, D), mine),
                      pl.BlockSpec((1, 1, GB), lambda j, sc: (sc[1] + j, 0, 0))] + [any_spec] * len(extra),
            out_specs=[pl.BlockSpec((GC, D), mine), pl.BlockSpec((GC, D), lambda j, sc: (j, 0)),
                       pl.BlockSpec((GC, 128), lambda j, sc: (j, 0))],
            scratch_shapes=[pltpu.VMEM((rows, D), jnp.bfloat16), pltpu.VMEM((D, rows), jnp.bfloat16),
                            pltpu.VMEM((8, rows), jnp.float32), pltpu.VMEM((8, rows), jnp.float32),
                            pltpu.VMEM((2, GC, GR), jnp.float32),
                            pltpu.VMEM((GC, GR), jnp.bfloat16), pltpu.VMEM((GB, 128), jnp.float32), pltpu.SemaphoreType.DMA((4,))]),
        out_shape=[jax.ShapeDtypeStruct((wt.shape[0], D), jnp.float32), jax.ShapeDtypeStruct((count * GC, D), jnp.float32),
                   jax.ShapeDtypeStruct((count * GC, 128), jnp.float32)],
        input_output_aliases={8: 0} if extra else {},
        compiler_params=pltpu.CompilerParams(dimension_semantics=("arbitrary",), vmem_limit_bytes=VMEM_LIMIT),
        cost_estimate=pl.CostEstimate(flops=4 * 8000 * D * count * GC, bytes_accessed=10 * D * count * GC,
                                      transcendentals=5400 * count * GC),
        name="grad_head",
    )(sc, wgt, zc, zt, lse, lab, wt, b_blk, *extra)


def place_kernel(blocks, vocab, at_ref, *refs):
    chunks, (out_ref, stage, in_sems, out_sems) = refs[:len(set(c for c, _ in blocks))], refs[-4:]
    slots = stage.shape[0]
    clip = vocab % GC

    def fetch(n):
        chunk, block = blocks[n]
        return pltpu.make_async_copy(chunks[chunk].at[pl.ds(block * GC, GC), :], stage.at[n % slots], in_sems.at[n % slots])

    def store(n, start, size):
        row = pl.multiple_of(at_ref[n] * GC, 8) + start
        return pltpu.make_async_copy(stage.at[n % slots, pl.ds(start, size), :], out_ref.at[pl.ds(row, size), :],
                                     out_sems.at[n % slots])

    def act(n, method):
        getattr(store(n, 0, clip), method)()

        @pl.when(at_ref[n] * GC + GC <= vocab)
        def _():
            getattr(store(n, clip, GC - clip), method)()

    for n in range(min(slots - 1, len(blocks))):
        fetch(n).start()
    for n in range(len(blocks)):
        fetch(n).wait()
        act(n, 'start')
        ahead = n + slots - 1
        if ahead < len(blocks):
            if n > 0:
                act(n - 1, 'wait')
            fetch(ahead).start()
    for n in range(max(len(blocks) - slots, 0), len(blocks)):
        act(n, 'wait')


def place(at, chunks, full):
    blocks = [(i, b) for i, chunk in enumerate(chunks) for b in range(chunk.shape[0] // GC)]
    any_spec = pl.BlockSpec(memory_space=pl.ANY)
    return pl.pallas_call(
        functools.partial(place_kernel, blocks, full.shape[0]),
        grid_spec=pltpu.PrefetchScalarGridSpec(
            num_scalar_prefetch=1, grid=(1,), in_specs=[any_spec] * (len(chunks) + 1), out_specs=any_spec,
            scratch_shapes=[pltpu.VMEM((6, GC, D), jnp.float32), pltpu.SemaphoreType.DMA((6,)),
                            pltpu.SemaphoreType.DMA((6,))]),
        out_shape=jax.ShapeDtypeStruct(full.shape, full.dtype),
        input_output_aliases={len(chunks) + 1: 0},
        compiler_params=pltpu.CompilerParams(dimension_semantics=("arbitrary",)),
        cost_estimate=pl.CostEstimate(flops=600 * GC * len(blocks) * D, bytes_accessed=8 * D * len(blocks) * GC,
                                      transcendentals=0),
        name="place",
    )(at, *chunks, full)


LN_EPS = 1e-5
ROPE_BASE = 10000.0
DATA_SPECS = (P('dp', None, None), P('dp', None), P('dp', None))
PARAM_SPECS = (P(None), P(None), P(None, 'tp', None), P(None, 'tp', None), P(None, 'tp', None),
               P('tp', None, None), P(None, 'tp'), P('tp'), P('tp', None), P(None), P(None), P(None),
               P(None, 'tp'), P('tp'))
SHARED = 2
PAIRED = 2


def norm_stats(values):
    row_mean = jnp.mean(values, axis=-1, keepdims=True)
    centered = values - row_mean
    inv_std = lax.rsqrt(jnp.mean(centered * centered, axis=-1, keepdims=True) + LN_EPS)
    return centered * inv_std, inv_std


def norm_backward(grad_out, x_hat, inv_std, gain_vec):
    grad_hat = grad_out * gain_vec
    mean_grad = jnp.mean(grad_hat, axis=-1, keepdims=True)
    mean_proj = jnp.mean(grad_hat * x_hat, axis=-1, keepdims=True)
    grad_in = inv_std * (grad_hat - mean_grad - x_hat * mean_proj)
    return grad_in, jnp.sum(grad_out * x_hat, axis=(0, 1)), jnp.sum(grad_out, axis=(0, 1))


def rope_tables(seq_count, rot_dim):
    half_rot = rot_dim // 2
    inv_freq = ROPE_BASE ** (-2.0 * jnp.arange(half_rot, dtype=jnp.float32) / rot_dim)
    angles = jnp.arange(seq_count, dtype=jnp.float32)[:, None] * inv_freq[None, :]
    return jnp.cos(angles)[:, None, :], jnp.sin(angles)[:, None, :]


def apply_rotary(tensor, cosine, sine_tab):
    rot_dim = 2 * cosine.shape[-1]
    pairs = tensor[..., :rot_dim].reshape(tensor.shape[:-1] + (rot_dim // 2, 2))
    even_part = pairs[..., 0]
    odd_part = pairs[..., 1]
    rotated = jnp.stack([even_part * cosine - odd_part * sine_tab, odd_part * cosine + even_part * sine_tab], axis=-1)
    return jnp.concatenate([rotated.reshape(tensor.shape[:-1] + (rot_dim,)), tensor[..., rot_dim:]], axis=-1)


TP_PAIRS = [(0, 1), (1, 0)]


def tp_sum(part):
    return part + lax.ppermute(part, 'tp', TP_PAIRS)


def dp_swap(array, mask):
    return lax.ppermute(array, 'dp', [(i, i ^ mask) for i in range(8)])


def offsets(lengths):
    padded = (lengths + 15) // 16 * 16
    return jnp.concatenate([jnp.zeros((1,), jnp.int32), jnp.cumsum(padded).astype(jnp.int32)])


def solution(mesh):
    def local_step(hidden, labels, loss_mask, ln_gain, ln_bias, w_query, w_key, w_value, w_attn_out,
                   w_fc_in, b_fc_in, w_fc_out, b_fc_out, lnf_gain, lnf_bias, w_head, b_head):
        seqs, seq_count = hidden.shape[:2]
        head_dim = w_query.shape[2]
        vocab_loc = w_head.shape[1]
        tp_idx, dp_idx = lax.axis_index('tp'), lax.axis_index('dp')
        score_scale = head_dim ** -0.5
        cosine, sine_tab = rope_tables(seq_count, head_dim // 4)
        causal = jnp.arange(seq_count)[None, :] <= jnp.arange(seq_count)[:, None]

        order = dp_idx ^ jnp.arange(8)
        off_own = offsets(jnp.sum(loss_mask, axis=-1))
        local_label = labels - tp_idx * vocab_loc
        in_local = (local_label >= 0) & (local_label < vocab_loc)
        safe_label = jnp.where(in_local, local_label, 0)
        wt_head = w_head.T
        b_row = jnp.pad(b_head, (0, -vocab_loc % FC), constant_values=PAD_BIAS)[None, :]
        n_blk = 8 * SHARED + 4 * PAIRED
        b_blk = jnp.pad(jnp.pad(b_head, (0, n_blk * GC - vocab_loc)).reshape(n_blk, 1, GC), ((0, 0), (0, 0), (0, GB - GC)))
        w_label = jnp.where(in_local[..., None], jnp.take(wt_head, safe_label, axis=0), 0).astype(jnp.float32)
        b_label = jnp.where(in_local, jnp.take(b_head, safe_label), 0.0)

        resid_in = hidden.astype(jnp.float32)
        ln_hat, ln_inv = norm_stats(resid_in)
        normed = (ln_hat * ln_gain + ln_bias).astype(jnp.bfloat16)
        q_rot = apply_rotary(jnp.einsum('btd,dhe->bthe', normed, w_query, preferred_element_type=jnp.float32),
                             cosine, sine_tab).astype(jnp.bfloat16)
        k_rot = apply_rotary(jnp.einsum('btd,dhe->bthe', normed, w_key, preferred_element_type=jnp.float32),
                             cosine, sine_tab).astype(jnp.bfloat16)
        v_proj = jnp.einsum('btd,dhe->bthe', normed, w_value, preferred_element_type=jnp.float32).astype(jnp.bfloat16)
        scores = jnp.einsum('bqhe,bkhe->bhqk', q_rot, k_rot, preferred_element_type=jnp.float32) * score_scale
        probs = jax.nn.softmax(jnp.where(causal, scores, -1e30), axis=-1)
        probs_bf = probs.astype(jnp.bfloat16)
        context = jnp.einsum('bhqk,bkhe->bqhe', probs_bf, v_proj, preferred_element_type=jnp.float32).astype(jnp.bfloat16)
        pre_act = jnp.einsum('btd,df->btf', normed, w_fc_in, preferred_element_type=jnp.float32) + b_fc_in
        gelu_out, gelu_vjp = jax.vjp(functools.partial(jax.nn.gelu, approximate=True), pre_act)
        gelu_bf = gelu_out.astype(jnp.bfloat16)
        block_part = (jnp.einsum('crif,ife->cre', context, w_attn_out, preferred_element_type=jnp.float32)
                      + jnp.einsum('btf,fd->btd', gelu_bf, w_fc_out, preferred_element_type=jnp.float32))
        resid_out = resid_in + tp_sum(block_part) + b_fc_out
        fin_hat, fin_inv = norm_stats(resid_out)
        final_bf = (fin_hat * lnf_gain + lnf_bias).astype(jnp.bfloat16)
        final_f32 = final_bf.astype(jnp.float32)

        half = seq_count // 2
        z_x, z_y = dp_swap(final_f32, 2), dp_swap(final_f32, 4)
        z_d0, z_d1 = dp_swap(z_x[:, :half], 4), dp_swap(z_y[:, half:], 2)
        pieces = [final_f32, dp_swap(final_f32, 1), z_x, dp_swap(z_x, 1), z_y, dp_swap(z_y, 1),
                  z_d0, z_d1, dp_swap(z_d0, 1), dp_swap(z_d1, 1)]

        u_part, m_b, s_b = head_forward(off_own, final_bf, w_head, wt_head, b_row)
        m_loc, s_loc = m_b[:, :, 0], s_b[:, :, 0]
        label_part = jnp.sum(final_f32 * w_label, axis=-1) + b_label
        stats = lax.all_gather(jnp.stack([m_loc, s_loc, label_part, labels.astype(jnp.float32),
                                          loss_mask.astype(jnp.float32)]), ('tp', 'dp'))
        stats = stats.reshape(2, 8, 5, seqs, seq_count)
        top = jnp.max(stats[:, :, 0], axis=0)
        lse_all = top + jnp.log(jnp.sum(stats[:, :, 1] * jnp.exp(stats[:, :, 0] - top), axis=0))
        valid = stats[0, :, 4] > 0
        lens_all = jnp.sum(stats[0, :, 4], axis=-1)
        inv_count = 1.0 / jnp.sum(lens_all)
        off_all = offsets(lens_all[order].reshape(-1).astype(jnp.int32))
        loss = jnp.sum(jnp.where(valid, lse_all - (stats[0, :, 2] + stats[1, :, 2]), 0.0)) * inv_count
        lse_own = lax.dynamic_index_in_dim(lse_all, dp_idx, 0, keepdims=False)
        own_valid = (loss_mask > 0)[..., None]
        scale = jnp.exp(m_loc - jnp.where(loss_mask > 0, lse_own, m_loc))[..., None]
        grad_final = tp_sum(jnp.where(own_valid, inv_count * (u_part * scale - w_label), 0.0))

        wide = lambda a: jnp.broadcast_to(a[order].reshape(8 * seqs, seq_count, 1), (8 * seqs, seq_count, 128))
        lse_wide = wide(jnp.where(valid, lse_all - jnp.log(inv_count), PAD_LSE))
        lab_wide = wide(jnp.where(valid, stats[0, :, 3] - (tp_idx * vocab_loc).astype(jnp.float32), PAD_LABEL))
        zc, zt, lse_c, lab_c = prep(off_all, pieces, lse_wide, lab_wide)
        core = lax.rem(dp_idx, 2)
        total = off_all[-1]
        wgt = inv_count.reshape(1)
        starts = lambda block: jnp.stack([total, block]).astype(jnp.int32)
        grad_rows = functools.partial(grad_head, wgt=wgt, zc=zc, zt=zt, lse=lse_c, lab=lab_c, wt=wt_head, b_blk=b_blk)
        full, g_own, bias_shared = grad_rows(SHARED, starts(dp_idx * SHARED))
        g_own, grad_final = lax.optimization_barrier((g_own, grad_final))
        g_x, g_y, g_core = dp_swap(g_own, 2), dp_swap(g_own, 4), dp_swap(g_own, 1)

        grad_resid, grad_lnf_gain, grad_lnf_bias = norm_backward(grad_final, fin_hat, fin_inv, lnf_gain)
        grad_b_fc_out = jnp.sum(grad_resid, axis=(0, 1))
        grad_block = grad_resid.astype(jnp.bfloat16)
        grad_w_fc_out = jnp.einsum('btf,btd->fd', gelu_bf, grad_block, preferred_element_type=jnp.float32)
        grad_gelu = jnp.einsum('btd,fd->btf', grad_block, w_fc_out, preferred_element_type=jnp.float32)
        grad_pre = gelu_vjp(grad_gelu)[0]
        grad_b_fc_in = jnp.sum(grad_pre, axis=(0, 1))
        grad_pre_bf = grad_pre.astype(jnp.bfloat16)
        grad_w_fc_in = jnp.einsum('btd,btf->df', normed, grad_pre_bf, preferred_element_type=jnp.float32)
        grad_w_attn_out = jnp.einsum('crif,cre->ife', context, grad_block, preferred_element_type=jnp.float32)
        grad_context = jnp.einsum('cre,ife->crif', grad_block, w_attn_out, preferred_element_type=jnp.float32).astype(jnp.bfloat16)
        grad_v = jnp.einsum('bhqk,bqhe->bkhe', probs_bf, grad_context, preferred_element_type=jnp.float32).astype(jnp.bfloat16)
        grad_probs = jnp.einsum('bqhe,bkhe->bhqk', grad_context, v_proj, preferred_element_type=jnp.float32)
        grad_scores = (probs * (grad_probs - jnp.sum(grad_probs * probs, axis=-1, keepdims=True)) * score_scale).astype(jnp.bfloat16)
        grad_q = apply_rotary(jnp.einsum('bhqk,bkhe->bqhe', grad_scores, k_rot, preferred_element_type=jnp.float32),
                              cosine, -sine_tab).astype(jnp.bfloat16)
        grad_k = apply_rotary(jnp.einsum('bhqk,bqhe->bkhe', grad_scores, q_rot, preferred_element_type=jnp.float32),
                              cosine, -sine_tab).astype(jnp.bfloat16)
        grad_w_query = jnp.einsum('btd,bthe->dhe', normed, grad_q, preferred_element_type=jnp.float32)
        grad_w_key = jnp.einsum('btd,bthe->dhe', normed, grad_k, preferred_element_type=jnp.float32)
        grad_w_value = jnp.einsum('btd,bthe->dhe', normed, grad_v, preferred_element_type=jnp.float32)
        grad_normed_part = (jnp.einsum('bthe,dhe->btd', grad_q, w_query, preferred_element_type=jnp.float32)
                             + jnp.einsum('bthe,dhe->btd', grad_k, w_key, preferred_element_type=jnp.float32)
                             + jnp.einsum('bthe,dhe->btd', grad_v, w_value, preferred_element_type=jnp.float32)
                             + jnp.einsum('btf,df->btd', grad_pre_bf, w_fc_in, preferred_element_type=jnp.float32))
        first = starts(8 * SHARED + core * 2 * PAIRED)
        first, grad_normed_part = lax.optimization_barrier((first, grad_normed_part))
        grad_normed_other = lax.ppermute(grad_normed_part, 'tp', TP_PAIRS)
        full, r_0, bias_0 = grad_rows(PAIRED, first, full=full)
        g_x, g_y, g_core, r_0, second = lax.optimization_barrier((g_x, g_y, g_core, r_0, first + jnp.array([0, PAIRED])))
        step = SHARED * GC // 2
        g_d0, g_d1 = dp_swap(g_x[:step], 4), dp_swap(g_y[step:], 2)
        g_x1, g_y1, r_0c = dp_swap(g_x, 1), dp_swap(g_y, 1), dp_swap(r_0, 1)
        full, r_1, bias_1 = grad_rows(PAIRED, second, full=full)
        r_1c = dp_swap(r_1, 1)
        shared_at = lambda mask: (dp_idx ^ mask) * SHARED
        pair_at = 8 * SHARED + (1 - core) * 2 * PAIRED
        full = place(jnp.stack([shared_at(m) + k for m in (1, 2, 4, 3, 5) for k in range(2)]
                               + [pair_at, pair_at + 1]).astype(jnp.int32), [g_core, g_x, g_y, g_x1, g_y1, r_0c], full)
        full = place(jnp.stack([shared_at(6), shared_at(6) + 1, shared_at(7), shared_at(7) + 1, pair_at + 2, pair_at + 3])
                     .astype(jnp.int32), [g_d0, g_d1, dp_swap(g_d0, 1), dp_swap(g_d1, 1), r_1c], full)
        grad_w_head = full.T
        bias_own = jnp.concatenate([jnp.sum(bias_0, axis=1), jnp.sum(bias_1, axis=1)])
        bias_other = dp_swap(bias_own, 1)
        bias_pair = jnp.where(core == 0, jnp.concatenate([bias_own, bias_other]), jnp.concatenate([bias_other, bias_own]))
        grad_normed = grad_normed_part + grad_normed_other
        grad_ln_in, grad_ln_gain, grad_ln_bias = norm_backward(grad_normed, ln_hat, ln_inv, ln_gain)
        grad_hidden = (grad_resid + grad_ln_in).astype(jnp.bfloat16)
        big = lax.psum((grad_w_query, grad_w_key, grad_w_value, grad_w_attn_out, grad_w_fc_in, grad_w_fc_out), 'dp')
        parts = [grad_ln_gain, grad_ln_bias, grad_b_fc_in, grad_b_fc_out, grad_lnf_gain, grad_lnf_bias]
        big, vector = lax.optimization_barrier((big, jnp.concatenate(parts + [jnp.sum(bias_shared, axis=1)])))
        gathered = lax.all_gather(vector, 'dp')
        n_small = sum(part.shape[0] for part in parts)
        sums = jnp.sum(gathered[:, :n_small], axis=0)
        small, at = [], 0
        for part in parts:
            small.append(sums[at:at + part.shape[0]])
            at += part.shape[0]
        grad_b_head = jnp.concatenate([gathered[:, n_small:].reshape(-1), bias_pair])[:vocab_loc]
        return (loss, grad_hidden, small[0], small[1], big[0], big[1], big[2], big[3], big[4], small[2], big[5],
                small[3], small[4], small[5], grad_w_head, grad_b_head)

    return jax.shard_map(local_step, mesh=mesh, in_specs=DATA_SPECS + PARAM_SPECS,
                         out_specs=(P(), P('dp', None, None)) + PARAM_SPECS, check_vma=False)
```

```python
import functools
import jax
import jax.numpy as jnp
from jax import lax
from jax.experimental import pallas as pl
from jax.experimental.pallas import tpu as pltpu
from jax.sharding import PartitionSpec as P

SEQ = 384
D = 512
FC = 2560
FR = 320
GC = 1056
GB = 1152
GS = 48
GR = 768
DEPTH = 6
PAD_BIAS = -3e38
PAD_LSE = 1e30
PAD_LABEL = -1e9
VMEM_LIMIT = 63 * 1024 * 1024


def head_kernel(first, last, tail, seqs, off_ref, z_ref, w_ref, wt_ref, b_ref, *refs):
    before, (u_ref, m_out, s_out, zc, acc, m_run, s_run, lbuf) = refs[:-8], refs[-8:]
    col = pl.program_id(0)
    n_rows = (off_ref[seqs] + FR - 1) // FR

    @pl.when(col == 0)
    def _():
        zc[...] = jnp.zeros_like(zc)
        for i in range(seqs):
            zc[pl.ds(pl.multiple_of(off_ref[i], 16), SEQ), :] = z_ref[i]
        if first:
            acc[...] = jnp.zeros_like(acc)
            s_run[...] = jnp.zeros_like(s_run)
            m_run[...] = jnp.full_like(m_run, PAD_BIAS)
        else:
            for held, old in zip((acc, m_run, s_run), before):
                held[...] = old[...]

    if last:
        @pl.when(col == pl.num_programs(0) - 1)
        def _():
            w_ref[:, tail:] = jnp.zeros((D, FC - tail), jnp.bfloat16)
            wt_ref[tail:, :] = jnp.zeros((FC - tail, D), jnp.bfloat16)

    def logits(step, slot):
        rows = pl.ds(pl.multiple_of(step * FR, FR), FR)
        lbuf[slot] = jnp.dot(zc[rows, :], w_ref[...], preferred_element_type=jnp.float32) + b_ref[...]

    def process(step, slot):
        rows = pl.ds(pl.multiple_of(step * FR, FR), FR)
        vals = lbuf[slot]
        m_old = m_run[rows, :]
        m_new = jnp.maximum(m_old, jnp.max(vals, axis=-1, keepdims=True))
        alpha = jnp.exp(m_old - m_new)
        parts = [jnp.exp(vals[:, c * 128:(c + 1) * 128] - m_new) for c in range(FC // 128)]
        s_run[rows, :] = s_run[rows, :] * alpha + functools.reduce(jnp.add, parts)
        m_run[rows, :] = m_new
        p = jnp.concatenate([part.astype(jnp.bfloat16) for part in parts], axis=-1)
        new = jnp.dot(p, wt_ref[...], preferred_element_type=jnp.float32)
        acc[rows, :] = acc[rows, :] * jnp.concatenate([alpha] * (D // 128), axis=-1) + new

    logits(0, 0)

    def body(step, carry):
        slot = lax.rem(step, 2)
        logits(step + 1, 1 - slot)
        process(step, slot)
        return carry

    lax.fori_loop(0, n_rows - 1, body, 0)
    process(n_rows - 1, lax.rem(n_rows - 1, 2))

    @pl.when(col == pl.num_programs(0) - 1)
    def _():
        if not last:
            u_ref[...], m_out[...], s_out[...] = acc[...], m_run[...], s_run[...]
        else:
            for i in range(seqs):
                rows = pl.ds(pl.multiple_of(off_ref[i], 16), SEQ)
                u_ref[i] = acc[rows, :]
                m_out[i] = m_run[rows, :]
                s_out[i] = jnp.broadcast_to(jnp.sum(s_run[rows, :], axis=-1, keepdims=True), (SEQ, 128))


def head_forward(block, count, off, z, w, wt, b, before=()):
    seqs = z.shape[0]
    vocab = wt.shape[0]
    n_col = pl.cdiv(vocab, FC)
    last = block + count == n_col
    rows = seqs * SEQ + 384
    rows = (rows + FR - 1) // FR * FR
    whole = lambda shape: pl.BlockSpec(shape, lambda j, off: (0,) * len(shape))
    outs = [(seqs, SEQ, D), (seqs, SEQ, 128), (seqs, SEQ, 128)] if last else [(rows, D), (rows, 128), (rows, 128)]
    return pl.pallas_call(
        functools.partial(head_kernel, block == 0, last, vocab - (n_col - 1) * FC, seqs),
        grid_spec=pltpu.PrefetchScalarGridSpec(
            num_scalar_prefetch=1,
            grid=(count,),
            in_specs=[whole((seqs, SEQ, D)), pl.BlockSpec((D, FC), lambda j, off: (0, block + j)),
                      pl.BlockSpec((FC, D), lambda j, off: (block + j, 0)),
                      pl.BlockSpec((1, FC), lambda j, off: (0, block + j))] + [whole(x.shape) for x in before],
            out_specs=[whole(shape) for shape in outs],
            scratch_shapes=[pltpu.VMEM((rows, D), jnp.bfloat16), pltpu.VMEM((rows, D), jnp.float32),
                            pltpu.VMEM((rows, 128), jnp.float32), pltpu.VMEM((rows, 128), jnp.float32),
                            pltpu.VMEM((2, FR, FC), jnp.float32)]),
        out_shape=[jax.ShapeDtypeStruct(shape, jnp.float32) for shape in outs],
        compiler_params=pltpu.CompilerParams(dimension_semantics=("arbitrary",), vmem_limit_bytes=VMEM_LIMIT),
        cost_estimate=pl.CostEstimate(flops=4 * 900 * D * FC * count, bytes_accessed=4 * D * FC * count,
                                      transcendentals=900 * FC * count),
        name="head_forward",
    )(off, z, w, wt, b, *before)


def prep_kernel(seqs, off_ref, *refs):
    (*pieces, lse_in, lab_in, zc_out, zt_out, lse_out, lab_out,
     stage, zc, zt, lse_v, lab_v, lse, lab, lse_t, lab_t, sems) = refs
    n_seq = seqs * 8
    half = SEQ // 2
    n_blk = (off_ref[n_seq] + GR - 1) // GR

    def fetch(seq):
        piece, row = divmod(seq, seqs)
        slot = seq % DEPTH
        if piece < 6:
            return [pltpu.make_async_copy(pieces[piece].at[row], stage.at[slot], sems.at[slot])]
        return [pltpu.make_async_copy(pieces[2 * piece - 6 + k].at[row], stage.at[slot, pl.ds(k * half, half)],
                                      sems.at[slot + DEPTH * k]) for k in range(2)]

    stats = [pltpu.make_async_copy(lse_in, lse_v, sems.at[2 * DEPTH]),
             pltpu.make_async_copy(lab_in, lab_v, sems.at[2 * DEPTH + 1])]
    for copy in sum((fetch(seq) for seq in range(DEPTH)), []) + stats:
        copy.start()
    zc[...] = jnp.zeros_like(zc)
    lse[...] = jnp.full_like(lse, PAD_LSE)
    lab[...] = jnp.full_like(lab, PAD_LABEL)
    for seq in range(n_seq):
        for copy in fetch(seq):
            copy.wait()
        zc[pl.ds(pl.multiple_of(off_ref[seq], 16), SEQ), :] = stage[seq % DEPTH].astype(jnp.bfloat16)
        if seq + DEPTH < n_seq:
            for copy in fetch(seq + DEPTH):
                copy.start()

    def out_z(step):
        rows = pl.ds(pl.multiple_of(step * GR, GR), GR)
        return [pltpu.make_async_copy(zc.at[rows, :], zc_out.at[rows, :], sems.at[0]),
                pltpu.make_async_copy(zt.at[:, rows], zt_out.at[:, rows], sems.at[1])]

    def out_stats(step):
        rows = pl.ds(pl.multiple_of(step * GR, GR), GR)
        return [pltpu.make_async_copy(lse_t.at[:, rows], lse_out.at[:, rows], sems.at[2]),
                pltpu.make_async_copy(lab_t.at[:, rows], lab_out.at[:, rows], sems.at[3])]

    def turn(step, carry):
        rows = pl.ds(pl.multiple_of(step * GR, GR), GR)
        zt[:, rows] = zc[rows, :].T
        for copy in out_z(step):
            copy.start()
        return carry

    lax.fori_loop(0, n_blk, turn, 0)
    for copy in stats:
        copy.wait()
    for seq in range(n_seq):
        rows = pl.ds(pl.multiple_of(off_ref[seq], 16), SEQ)
        lse[rows, :] = lse_v[seq]
        lab[rows, :] = lab_v[seq]

    def send(step, carry):
        rows = pl.ds(pl.multiple_of(step * GR, GR), GR)
        lse_t[:, rows] = lse[rows, :].T[:8]
        lab_t[:, rows] = lab[rows, :].T[:8]
        for copy in out_stats(step):
            copy.start()
        return carry

    def finish(step, carry):
        for copy in out_z(step) + out_stats(step):
            copy.wait()
        return carry

    lax.fori_loop(0, n_blk, send, 0)
    lax.fori_loop(0, n_blk, finish, 0)


def prep(off, pieces, lse, lab):
    n_seq = lse.shape[0]
    rows = n_seq * SEQ
    any_spec = pl.BlockSpec(memory_space=pl.ANY)
    return pl.pallas_call(
        functools.partial(prep_kernel, n_seq // 8),
        grid_spec=pltpu.PrefetchScalarGridSpec(
            num_scalar_prefetch=1, grid=(1,), in_specs=[any_spec] * (len(pieces) + 2), out_specs=[any_spec] * 4,
            scratch_shapes=[pltpu.VMEM((DEPTH, SEQ, D), jnp.float32), pltpu.VMEM((rows, D), jnp.bfloat16),
                            pltpu.VMEM((D, rows), jnp.bfloat16), pltpu.VMEM((n_seq, SEQ, 128), jnp.float32),
                            pltpu.VMEM((n_seq, SEQ, 128), jnp.float32), pltpu.VMEM((rows, 128), jnp.float32),
                            pltpu.VMEM((rows, 128), jnp.float32), pltpu.VMEM((8, rows), jnp.float32),
                            pltpu.VMEM((8, rows), jnp.float32), pltpu.SemaphoreType.DMA((2 * DEPTH + 2,))]),
        out_shape=[jax.ShapeDtypeStruct((rows, D), jnp.bfloat16), jax.ShapeDtypeStruct((D, rows), jnp.bfloat16),
                   jax.ShapeDtypeStruct((8, rows), jnp.float32), jax.ShapeDtypeStruct((8, rows), jnp.float32)],
        compiler_params=pltpu.CompilerParams(dimension_semantics=("arbitrary",), vmem_limit_bytes=VMEM_LIMIT),
        cost_estimate=pl.CostEstimate(flops=400 * rows * 128, bytes_accessed=8 * rows * D, transcendentals=0),
        name="prep",
    )(off, *pieces, lse, lab)


def grad_head_kernel(sc_ref, wgt_ref, z_hbm, zt_hbm, lse_hbm, lab_hbm, wt_ref, b_ref, *refs):
    (out_ref, send_ref, gb_ref, zc, zt, lse, lab, lbuf, pbuf, bias, sems) = refs[-11:]
    j = pl.program_id(0)
    n_blk = (sc_ref[0] + GR - 1) // GR
    row0 = ((sc_ref[1] + j) * GC).astype(jnp.float32)
    weight = wgt_ref[0]

    @pl.when(j == 0)
    def _():
        def copies(step):
            cols = pl.ds(pl.multiple_of(step * GR, GR), GR)
            return [pltpu.make_async_copy(z_hbm.at[cols, :], zc.at[cols, :], sems.at[0]),
                    pltpu.make_async_copy(zt_hbm.at[:, cols], zt.at[:, cols], sems.at[1]),
                    pltpu.make_async_copy(lse_hbm.at[:, cols], lse.at[:, cols], sems.at[2]),
                    pltpu.make_async_copy(lab_hbm.at[:, cols], lab.at[:, cols], sems.at[3])]

        def start(step, carry):
            for copy in copies(step):
                copy.start()
            return carry

        def wait(step, carry):
            for copy in copies(step):
                copy.wait()
            return carry
        lax.fori_loop(0, n_blk, start, 0)
        lax.fori_loop(0, n_blk, wait, 0)

    iota = lax.broadcasted_iota(jnp.int32, (GS, 128), 0).astype(jnp.float32)
    for c in range(GB // 128):
        cols = slice(c * 128, (c + 1) * 128)
        bias[cols, :] = jnp.broadcast_to(b_ref[0, :, cols], (128, 128)).T

    def logits(step, slot):
        cols = pl.ds(pl.multiple_of(step * GR, GR), GR)
        lbuf[slot] = jnp.dot(wt_ref[...], zt[:, cols], preferred_element_type=jnp.float32)

    def process(step, slot):
        for s in range(GC // GS):
            strip = slice(s * GS, (s + 1) * GS)
            shift = bias[strip, :]
            total = None
            for c in range(GR // 128):
                cols = pl.ds(pl.multiple_of(step * GR + c * 128, 128), 128)
                p = jnp.exp(lbuf[slot, strip, c * 128:(c + 1) * 128] + shift - lse[0:1, cols])
                p = jnp.where(iota == lab[0:1, cols] - (row0 + s * GS), p - weight, p)
                total = p if total is None else total + p
                pbuf[strip, c * 128:(c + 1) * 128] = p.astype(jnp.bfloat16)
            gb_ref[strip, :] += total
        rows = pl.ds(pl.multiple_of(step * GR, GR), GR)
        out_ref[...] += jnp.dot(pbuf[...], zc[rows, :], preferred_element_type=jnp.float32)

    out_ref[...] = jnp.zeros_like(out_ref)
    gb_ref[...] = jnp.zeros_like(gb_ref)
    logits(0, 0)

    def body(step, carry):
        slot = lax.rem(step, 2)
        logits(step + 1, 1 - slot)
        process(step, slot)
        return carry

    lax.fori_loop(0, n_blk - 1, body, 0)
    process(n_blk - 1, lax.rem(n_blk - 1, 2))
    send_ref[...] = out_ref[...]


def grad_head(count, sc, wgt, zc, zt, lse, lab, wt, b_blk, full=None):
    rows = zc.shape[0]
    any_spec = pl.BlockSpec(memory_space=pl.ANY)
    smem = pl.BlockSpec(memory_space=pltpu.SMEM)
    extra = [] if full is None else [full]
    mine = lambda j, sc: (sc[1] + j, 0)
    return pl.pallas_call(
        grad_head_kernel,
        grid_spec=pltpu.PrefetchScalarGridSpec(
            num_scalar_prefetch=1, grid=(count,),
            in_specs=[smem, any_spec, any_spec, any_spec, any_spec, pl.BlockSpec((GC, D), mine),
                      pl.BlockSpec((1, 1, GB), lambda j, sc: (sc[1] + j, 0, 0))] + [any_spec] * len(extra),
            out_specs=[pl.BlockSpec((GC, D), mine), pl.BlockSpec((GC, D), lambda j, sc: (j, 0)),
                       pl.BlockSpec((GC, 128), lambda j, sc: (j, 0))],
            scratch_shapes=[pltpu.VMEM((rows, D), jnp.bfloat16), pltpu.VMEM((D, rows), jnp.bfloat16),
                            pltpu.VMEM((8, rows), jnp.float32), pltpu.VMEM((8, rows), jnp.float32),
                            pltpu.VMEM((2, GC, GR), jnp.float32),
                            pltpu.VMEM((GC, GR), jnp.bfloat16), pltpu.VMEM((GB, 128), jnp.float32), pltpu.SemaphoreType.DMA((4,))]),
        out_shape=[jax.ShapeDtypeStruct((wt.shape[0], D), jnp.float32), jax.ShapeDtypeStruct((count * GC, D), jnp.float32),
                   jax.ShapeDtypeStruct((count * GC, 128), jnp.float32)],
        input_output_aliases={8: 0} if extra else {},
        compiler_params=pltpu.CompilerParams(dimension_semantics=("arbitrary",), vmem_limit_bytes=VMEM_LIMIT),
        cost_estimate=pl.CostEstimate(flops=4 * 8000 * D * count * GC, bytes_accessed=10 * D * count * GC,
                                      transcendentals=5400 * count * GC),
        name="grad_head",
    )(sc, wgt, zc, zt, lse, lab, wt, b_blk, *extra)


def place_kernel(blocks, vocab, at_ref, *refs):
    chunks, (out_ref, stage, in_sems, out_sems) = refs[:len(set(c for c, _ in blocks))], refs[-4:]
    slots = stage.shape[0]
    clip = vocab % GC

    def fetch(n):
        chunk, block = blocks[n]
        return pltpu.make_async_copy(chunks[chunk].at[pl.ds(block * GC, GC), :], stage.at[n % slots], in_sems.at[n % slots])

    def store(n, start, size):
        row = pl.multiple_of(at_ref[n] * GC, 8) + start
        return pltpu.make_async_copy(stage.at[n % slots, pl.ds(start, size), :], out_ref.at[pl.ds(row, size), :],
                                     out_sems.at[n % slots])

    def act(n, method):
        getattr(store(n, 0, clip), method)()

        @pl.when(at_ref[n] * GC + GC <= vocab)
        def _():
            getattr(store(n, clip, GC - clip), method)()

    for n in range(min(slots - 1, len(blocks))):
        fetch(n).start()
    for n in range(len(blocks)):
        fetch(n).wait()
        act(n, 'start')
        ahead = n + slots - 1
        if ahead < len(blocks):
            if n > 0:
                act(n - 1, 'wait')
            fetch(ahead).start()
    for n in range(max(len(blocks) - slots, 0), len(blocks)):
        act(n, 'wait')


def place(at, chunks, full):
    blocks = [(i, b) for i, chunk in enumerate(chunks) for b in range(chunk.shape[0] // GC)]
    any_spec = pl.BlockSpec(memory_space=pl.ANY)
    return pl.pallas_call(
        functools.partial(place_kernel, blocks, full.shape[0]),
        grid_spec=pltpu.PrefetchScalarGridSpec(
            num_scalar_prefetch=1, grid=(1,), in_specs=[any_spec] * (len(chunks) + 1), out_specs=any_spec,
            scratch_shapes=[pltpu.VMEM((6, GC, D), jnp.float32), pltpu.SemaphoreType.DMA((6,)),
                            pltpu.SemaphoreType.DMA((6,))]),
        out_shape=jax.ShapeDtypeStruct(full.shape, full.dtype),
        input_output_aliases={len(chunks) + 1: 0},
        compiler_params=pltpu.CompilerParams(dimension_semantics=("arbitrary",)),
        cost_estimate=pl.CostEstimate(flops=600 * GC * len(blocks) * D, bytes_accessed=8 * D * len(blocks) * GC,
                                      transcendentals=0),
        name="place",
    )(at, *chunks, full)


LN_EPS = 1e-5
ROPE_BASE = 10000.0
DATA_SPECS = (P('dp', None, None), P('dp', None), P('dp', None))
PARAM_SPECS = (P(None), P(None), P(None, 'tp', None), P(None, 'tp', None), P(None, 'tp', None),
               P('tp', None, None), P(None, 'tp'), P('tp'), P('tp', None), P(None), P(None), P(None),
               P(None, 'tp'), P('tp'))
SHARED = 2
HEAD_FIRST = 7
PAIRED = 2


def norm_stats(values):
    row_mean = jnp.mean(values, axis=-1, keepdims=True)
    centered = values - row_mean
    inv_std = lax.rsqrt(jnp.mean(centered * centered, axis=-1, keepdims=True) + LN_EPS)
    return centered * inv_std, inv_std


def norm_backward(grad_out, x_hat, inv_std, gain_vec):
    grad_hat = grad_out * gain_vec
    mean_grad = jnp.mean(grad_hat, axis=-1, keepdims=True)
    mean_proj = jnp.mean(grad_hat * x_hat, axis=-1, keepdims=True)
    grad_in = inv_std * (grad_hat - mean_grad - x_hat * mean_proj)
    return grad_in, jnp.sum(grad_out * x_hat, axis=(0, 1)), jnp.sum(grad_out, axis=(0, 1))


def rope_tables(seq_count, rot_dim):
    half_rot = rot_dim // 2
    inv_freq = ROPE_BASE ** (-2.0 * jnp.arange(half_rot, dtype=jnp.float32) / rot_dim)
    angles = jnp.arange(seq_count, dtype=jnp.float32)[:, None] * inv_freq[None, :]
    return jnp.cos(angles)[:, None, :], jnp.sin(angles)[:, None, :]


def apply_rotary(tensor, cosine, sine_tab):
    rot_dim = 2 * cosine.shape[-1]
    pairs = tensor[..., :rot_dim].reshape(tensor.shape[:-1] + (rot_dim // 2, 2))
    even_part = pairs[..., 0]
    odd_part = pairs[..., 1]
    rotated = jnp.stack([even_part * cosine - odd_part * sine_tab, odd_part * cosine + even_part * sine_tab], axis=-1)
    return jnp.concatenate([rotated.reshape(tensor.shape[:-1] + (rot_dim,)), tensor[..., rot_dim:]], axis=-1)


TP_PAIRS = [(0, 1), (1, 0)]


def tp_sum(part):
    return part + lax.ppermute(part, 'tp', TP_PAIRS)


def dp_swap(array, mask):
    return lax.ppermute(array, 'dp', [(i, i ^ mask) for i in range(8)])


def offsets(lengths):
    padded = (lengths + 15) // 16 * 16
    return jnp.concatenate([jnp.zeros((1,), jnp.int32), jnp.cumsum(padded).astype(jnp.int32)])


def solution(mesh):
    def local_step(hidden, labels, loss_mask, ln_gain, ln_bias, w_query, w_key, w_value, w_attn_out,
                   w_fc_in, b_fc_in, w_fc_out, b_fc_out, lnf_gain, lnf_bias, w_head, b_head):
        seqs, seq_count = hidden.shape[:2]
        head_dim = w_query.shape[2]
        vocab_loc = w_head.shape[1]
        tp_idx, dp_idx = lax.axis_index('tp'), lax.axis_index('dp')
        score_scale = head_dim ** -0.5
        cosine, sine_tab = rope_tables(seq_count, head_dim // 4)
        causal = jnp.arange(seq_count)[None, :] <= jnp.arange(seq_count)[:, None]

        order = dp_idx ^ jnp.arange(8)
        off_own = offsets(jnp.sum(loss_mask, axis=-1))
        local_label = labels - tp_idx * vocab_loc
        in_local = (local_label >= 0) & (local_label < vocab_loc)
        safe_label = jnp.where(in_local, local_label, 0)
        wt_head = w_head.T
        b_row = jnp.pad(b_head, (0, -vocab_loc % FC), constant_values=PAD_BIAS)[None, :]
        n_blk = 8 * SHARED + 4 * PAIRED
        b_blk = jnp.pad(jnp.pad(b_head, (0, n_blk * GC - vocab_loc)).reshape(n_blk, 1, GC), ((0, 0), (0, 0), (0, GB - GC)))
        w_label = jnp.where(in_local[..., None], jnp.take(wt_head, safe_label, axis=0), 0).astype(jnp.float32)
        b_label = jnp.where(in_local, jnp.take(b_head, safe_label), 0.0)

        resid_in = hidden.astype(jnp.float32)
        ln_hat, ln_inv = norm_stats(resid_in)
        normed = (ln_hat * ln_gain + ln_bias).astype(jnp.bfloat16)
        q_rot = apply_rotary(jnp.einsum('btd,dhe->bthe', normed, w_query, preferred_element_type=jnp.float32),
                             cosine, sine_tab).astype(jnp.bfloat16)
        k_rot = apply_rotary(jnp.einsum('btd,dhe->bthe', normed, w_key, preferred_element_type=jnp.float32),
                             cosine, sine_tab).astype(jnp.bfloat16)
        v_proj = jnp.einsum('btd,dhe->bthe', normed, w_value, preferred_element_type=jnp.float32).astype(jnp.bfloat16)
        scores = jnp.einsum('bqhe,bkhe->bhqk', q_rot, k_rot, preferred_element_type=jnp.float32) * score_scale
        probs = jax.nn.softmax(jnp.where(causal, scores, -1e30), axis=-1)
        probs_bf = probs.astype(jnp.bfloat16)
        context = jnp.einsum('bhqk,bkhe->bqhe', probs_bf, v_proj, preferred_element_type=jnp.float32).astype(jnp.bfloat16)
        pre_act = jnp.einsum('btd,df->btf', normed, w_fc_in, preferred_element_type=jnp.float32) + b_fc_in
        gelu_out, gelu_vjp = jax.vjp(functools.partial(jax.nn.gelu, approximate=True), pre_act)
        gelu_bf = gelu_out.astype(jnp.bfloat16)
        block_part = (jnp.einsum('crif,ife->cre', context, w_attn_out, preferred_element_type=jnp.float32)
                      + jnp.einsum('btf,fd->btd', gelu_bf, w_fc_out, preferred_element_type=jnp.float32))
        resid_out = resid_in + tp_sum(block_part) + b_fc_out
        fin_hat, fin_inv = norm_stats(resid_out)
        final_bf = (fin_hat * lnf_gain + lnf_bias).astype(jnp.bfloat16)
        final_f32 = final_bf.astype(jnp.float32)

        half = seq_count // 2
        z_x, z_y = dp_swap(final_f32, 2), dp_swap(final_f32, 4)
        state = head_forward(0, HEAD_FIRST, off_own, final_bf, w_head, wt_head, b_row)
        z_x, z_y, from_x, from_y, state = lax.optimization_barrier((z_x, z_y, z_x[:, :half], z_y[:, half:], state))
        z_d0, z_d1 = dp_swap(from_x, 4), dp_swap(from_y, 2)
        pieces = [final_f32, dp_swap(final_f32, 1), z_x, dp_swap(z_x, 1), z_y, dp_swap(z_y, 1),
                  z_d0, z_d1, dp_swap(z_d0, 1), dp_swap(z_d1, 1)]

        u_part, m_b, s_b = head_forward(HEAD_FIRST, -(-vocab_loc // FC) - HEAD_FIRST, off_own, final_bf, w_head, wt_head, b_row, state)
        m_loc, s_loc = m_b[:, :, 0], s_b[:, :, 0]
        label_part = jnp.sum(final_f32 * w_label, axis=-1) + b_label
        mine = jnp.stack([m_loc, s_loc, label_part])
        other = lax.ppermute(mine, 'tp', TP_PAIRS)
        top = jnp.maximum(m_loc, other[0])
        lse_own = top + jnp.log(s_loc * jnp.exp(m_loc - top) + other[1] * jnp.exp(other[0] - top))
        own_valid = loss_mask > 0
        scale = jnp.exp(m_loc - jnp.where(own_valid, lse_own, m_loc))[..., None]
        grad_final = tp_sum(jnp.where(own_valid[..., None], u_part * scale - w_label, 0.0))
        stats = jnp.stack([lse_own, labels.astype(jnp.float32), loss_mask.astype(jnp.float32), label_part + other[2]])[None]
        for mask in (1, 2, 4):
            stats = jnp.concatenate([stats, dp_swap(stats, mask)])
        valid = stats[:, 2] > 0
        lens_all = jnp.sum(stats[:, 2], axis=-1)
        inv_count = 1.0 / jnp.sum(lens_all)
        off_all = offsets(lens_all.reshape(-1).astype(jnp.int32))
        piece_loss = jnp.sum(jnp.where(valid, stats[:, 0] - stats[:, 3], 0.0), axis=(1, 2))
        loss = jnp.sum(piece_loss[order]) * inv_count
        grad_final = grad_final * inv_count

        wide = lambda a: jnp.broadcast_to(a.reshape(8 * seqs, seq_count, 1), (8 * seqs, seq_count, 128))
        lse_wide = wide(jnp.where(valid, stats[:, 0] - jnp.log(inv_count), PAD_LSE))
        lab_wide = wide(jnp.where(valid, stats[:, 1] - (tp_idx * vocab_loc).astype(jnp.float32), PAD_LABEL))
        zc, zt, lse_c, lab_c = prep(off_all, pieces, lse_wide, lab_wide)
        core = lax.rem(dp_idx, 2)
        total = off_all[-1]
        wgt = inv_count.reshape(1)
        starts = lambda block: jnp.stack([total, block]).astype(jnp.int32)
        grad_rows = functools.partial(grad_head, wgt=wgt, zc=zc, zt=zt, lse=lse_c, lab=lab_c, wt=wt_head, b_blk=b_blk)
        full, g_own, bias_shared = grad_rows(SHARED, starts(dp_idx * SHARED))
        g_own, grad_final = lax.optimization_barrier((g_own, grad_final))
        g_x, g_y, g_core = dp_swap(g_own, 2), dp_swap(g_own, 4), dp_swap(g_own, 1)

        grad_resid, grad_lnf_gain, grad_lnf_bias = norm_backward(grad_final, fin_hat, fin_inv, lnf_gain)
        grad_b_fc_out = jnp.sum(grad_resid, axis=(0, 1))
        grad_block = grad_resid.astype(jnp.bfloat16)
        grad_w_fc_out = jnp.einsum('btf,btd->fd', gelu_bf, grad_block, preferred_element_type=jnp.float32)
        grad_gelu = jnp.einsum('btd,fd->btf', grad_block, w_fc_out, preferred_element_type=jnp.float32)
        grad_pre = gelu_vjp(grad_gelu)[0]
        grad_b_fc_in = jnp.sum(grad_pre, axis=(0, 1))
        grad_pre_bf = grad_pre.astype(jnp.bfloat16)
        grad_w_fc_in = jnp.einsum('btd,btf->df', normed, grad_pre_bf, preferred_element_type=jnp.float32)
        grad_w_attn_out = jnp.einsum('crif,cre->ife', context, grad_block, preferred_element_type=jnp.float32)
        grad_context = jnp.einsum('cre,ife->crif', grad_block, w_attn_out, preferred_element_type=jnp.float32).astype(jnp.bfloat16)
        grad_v = jnp.einsum('bhqk,bqhe->bkhe', probs_bf, grad_context, preferred_element_type=jnp.float32).astype(jnp.bfloat16)
        grad_probs = jnp.einsum('bqhe,bkhe->bhqk', grad_context, v_proj, preferred_element_type=jnp.float32)
        grad_scores = (probs * (grad_probs - jnp.sum(grad_probs * probs, axis=-1, keepdims=True)) * score_scale).astype(jnp.bfloat16)
        grad_q = apply_rotary(jnp.einsum('bhqk,bkhe->bqhe', grad_scores, k_rot, preferred_element_type=jnp.float32),
                              cosine, -sine_tab).astype(jnp.bfloat16)
        grad_k = apply_rotary(jnp.einsum('bhqk,bqhe->bkhe', grad_scores, q_rot, preferred_element_type=jnp.float32),
                              cosine, -sine_tab).astype(jnp.bfloat16)
        grad_w_query = jnp.einsum('btd,bthe->dhe', normed, grad_q, preferred_element_type=jnp.float32)
        grad_w_key = jnp.einsum('btd,bthe->dhe', normed, grad_k, preferred_element_type=jnp.float32)
        grad_w_value = jnp.einsum('btd,bthe->dhe', normed, grad_v, preferred_element_type=jnp.float32)
        grad_normed_part = (jnp.einsum('bthe,dhe->btd', grad_q, w_query, preferred_element_type=jnp.float32)
                             + jnp.einsum('bthe,dhe->btd', grad_k, w_key, preferred_element_type=jnp.float32)
                             + jnp.einsum('bthe,dhe->btd', grad_v, w_value, preferred_element_type=jnp.float32)
                             + jnp.einsum('btf,df->btd', grad_pre_bf, w_fc_in, preferred_element_type=jnp.float32))
        first = starts(8 * SHARED + core * 2 * PAIRED)
        first, grad_normed_part = lax.optimization_barrier((first, grad_normed_part))
        grad_normed_other = lax.ppermute(grad_normed_part, 'tp', TP_PAIRS)
        full, r_0, bias_0 = grad_rows(PAIRED, first, full=full)
        g_x, g_y, g_core, r_0, second = lax.optimization_barrier((g_x, g_y, g_core, r_0, first + jnp.array([0, PAIRED])))
        step = SHARED * GC // 2
        g_d0, g_d1 = dp_swap(g_x[:step], 4), dp_swap(g_y[step:], 2)
        g_x1, g_y1, r_0c = dp_swap(g_x, 1), dp_swap(g_y, 1), dp_swap(r_0, 1)
        full, r_1, bias_1 = grad_rows(PAIRED, second, full=full)
        r_1c = dp_swap(r_1, 1)
        shared_at = lambda mask: (dp_idx ^ mask) * SHARED
        pair_at = 8 * SHARED + (1 - core) * 2 * PAIRED
        full = place(jnp.stack([shared_at(m) + k for m in (1, 2, 4, 3, 5) for k in range(2)]
                               + [pair_at, pair_at + 1]).astype(jnp.int32), [g_core, g_x, g_y, g_x1, g_y1, r_0c], full)
        full = place(jnp.stack([shared_at(6), shared_at(6) + 1, shared_at(7), shared_at(7) + 1, pair_at + 2, pair_at + 3])
                     .astype(jnp.int32), [g_d0, g_d1, dp_swap(g_d0, 1), dp_swap(g_d1, 1), r_1c], full)
        grad_w_head = full.T
        bias_own = jnp.concatenate([jnp.sum(bias_0, axis=1), jnp.sum(bias_1, axis=1)])
        bias_other = dp_swap(bias_own, 1)
        bias_pair = jnp.where(core == 0, jnp.concatenate([bias_own, bias_other]), jnp.concatenate([bias_other, bias_own]))
        grad_normed = grad_normed_part + grad_normed_other
        grad_ln_in, grad_ln_gain, grad_ln_bias = norm_backward(grad_normed, ln_hat, ln_inv, ln_gain)
        grad_hidden = (grad_resid + grad_ln_in).astype(jnp.bfloat16)
        big = lax.psum((grad_w_query, grad_w_key, grad_w_value, grad_w_attn_out, grad_w_fc_in, grad_w_fc_out), 'dp')
        parts = [grad_ln_gain, grad_ln_bias, grad_b_fc_in, grad_b_fc_out, grad_lnf_gain, grad_lnf_bias]
        sums = jnp.concatenate(parts)
        for mask in (1, 2, 4):
            sums = sums + dp_swap(sums, mask)
        small, at = [], 0
        for part in parts:
            small.append(sums[at:at + part.shape[0]])
            at += part.shape[0]
        bias_all = jnp.sum(bias_shared, axis=1)[None]
        for mask in (1, 2, 4):
            bias_all = jnp.concatenate([bias_all, dp_swap(bias_all, mask)])
        grad_b_head = jnp.concatenate([bias_all[order].reshape(-1), bias_pair])[:vocab_loc]
        return (loss, grad_hidden, small[0], small[1], big[0], big[1], big[2], big[3], big[4], small[2], big[5],
                small[3], small[4], small[5], grad_w_head, grad_b_head)

    return jax.shard_map(local_step, mesh=mesh, in_specs=DATA_SPECS + PARAM_SPECS,
                         out_specs=(P(), P('dp', None, None)) + PARAM_SPECS, check_vma=False)
```
